32 devices in a mesh: dp: 8 (over z, y), tp: 4 (over x, core).
Axes of the slice: x: 2, y: 2, z: 4, core: 2. Of those that a mesh axis runs over, the one named last changes fastest.
Arguments:
- queries: bfloat16 [64, 16, 8192], P(('dp', 'tp')), parts along dimension 0, may hold values from -512 to 512
- kv_cache: bfloat16 [64, 8, 384, 256], P(('dp', 'tp')), parts along dimension 0, may hold values from -18 to 18
- lengths: int32 [64], P(('dp', 'tp')), parts along dimension 0, may hold values from 17 to 384, as said below
- residual: bfloat16 [64, 16, 8192], P(('dp', 'tp')), parts along dimension 0, may hold values from -4 to 4
- out_weight: bfloat16 [8192, 8192], P('tp'), may hold values from -0.0625 to 0.0625
- norm_gain: bfloat16 [8192], replicated, may hold values from 0.25 to 1.75
Outputs:
- hidden: bfloat16 [64, 16, 8192], P(('dp', 'tp')), parts along dimension 0
- normed: bfloat16 [64, 16, 8192], P(('dp', 'tp')), parts along dimension 0
The draws below stay inside these ranges and needn't reach their ends.
There are 8 independent parts, one for each index of `dp`. The reference program is written for one: setup_inputs(seed, part) draws one part's arguments, and reference() takes and returns one part's arrays. A program takes and returns all parts, laid end to end along the dimension named above; an argument that names none is the same for every part. Nothing has to cross between parts.
Inputs may be any that keep to these rules, and one draw needn't show every extreme that they name: `lengths`: some sequence of every part has exactly 384 live slots.
All inputs are finite; a program needn't handle non-finite values.
Results may differ from the reference program's by a relative error of at most 0.015.
Values may be sent and summed in bfloat16 or wider, within the bound.
No kernel may reach another device: no remote copies, remote signals or barrier semaphores. Data moves between devices by JAX's collectives and lax.ppermute only.
A program may use at most 128 MiB of HBM per device.

```python
import jax
import jax.numpy as jnp
from jax import lax

D = 8192
HEADS = 64
KV_HEADS = 8
HEAD_DIM = 128
DRAFT = 16
LEN = 384
SEQS = 8
N_TP = 4


def draw_queries(key, part):
    normal_part = jnp.clip(jax.random.normal(jax.random.fold_in(key, 11), (SEQS, DRAFT, HEADS * HEAD_DIM), jnp.float32) * 1.5, -9.0, 9.0)
    return normal_part.astype(jnp.bfloat16)


def draw_kv_cache(key, part):
    shape_all = (SEQS, KV_HEADS, LEN, HEAD_DIM)
    key_part = jnp.clip(jax.random.normal(jax.random.fold_in(key, 21), shape_all, jnp.float32), -6.0, 6.0)
    value_part = jnp.clip(jax.random.normal(jax.random.fold_in(key, 22), shape_all, jnp.float32) * 3.0, -18.0, 18.0)
    return jnp.concatenate([key_part, value_part], axis=-1).astype(jnp.bfloat16)


def draw_lengths(key, part):
    drawn = jax.random.randint(jax.random.fold_in(key, 31), (SEQS,), DRAFT + 1, LEN + 1, dtype=jnp.int32)
    return drawn.at[0].set(LEN)


def draw_residual(key, part):
    row_values = jax.random.normal(jax.random.fold_in(key, 41), (SEQS, DRAFT, D), jnp.float32) * 0.5
    return jnp.clip(row_values, -4.0, 4.0).astype(jnp.bfloat16)


def block_scale(own_key, extent, cuts, smallest, top_value):
    loudness, own = 1.0, jax.random.fold_in(own_key, 6)
    for dim, parts in cuts:
        heights = jnp.exp(jax.random.uniform(jax.random.fold_in(own, dim), (parts,), jnp.float32, smallest / len(cuts), top_value / len(cuts)))
        loudness = loudness * jnp.repeat(heights, extent[dim] // parts).reshape([-1 if axis == dim else 1 for axis in range(len(extent))])
    return loudness


def gaussian(key, extent, width, most, shards=(), kind=jnp.bfloat16):
    gain = block_scale(key, extent, shards, -0.22, 0.18) if shards else 1.0
    entries = jax.random.normal(key, extent, jnp.float32) * width * gain
    return jnp.minimum(jnp.maximum(entries, -most), most).astype(kind)


def setup_inputs(seed: int = 0, part: int = 0) -> dict:
    key_list = jax.random.split(jax.random.key(seed), 7)
    own_keys = jax.random.split(jax.random.fold_in(key_list[6], part), 7)
    return {
        "queries": draw_queries(jax.random.fold_in(jax.random.fold_in(key_list[6], part), 71), part),
        "kv_cache": draw_kv_cache(jax.random.fold_in(jax.random.fold_in(key_list[6], part), 71), part),
        "lengths": draw_lengths(jax.random.fold_in(jax.random.fold_in(key_list[6], part), 71), part),
        "residual": draw_residual(jax.random.fold_in(jax.random.fold_in(key_list[6], part), 71), part),
        "out_weight": gaussian(key_list[4], (HEADS * HEAD_DIM, D), (HEADS * HEAD_DIM) ** -0.5, 0.0625, ((0, 4),)),
        "norm_gain": jnp.clip(1.0 + 0.15 * jax.random.normal(key_list[5], (D,), jnp.float32), 0.25, 1.75).astype(jnp.bfloat16),
    }


def attend(queries, kv_cache, lengths):
    seq_count = queries.shape[0]
    per_group = HEADS // KV_HEADS
    grouped = queries.reshape(seq_count, DRAFT, KV_HEADS, per_group, HEAD_DIM).transpose(0, 2, 3, 1, 4)
    grouped = grouped.reshape(seq_count, KV_HEADS, per_group * DRAFT, HEAD_DIM).astype(jnp.float32)
    key_part = kv_cache[..., :HEAD_DIM].astype(jnp.float32)
    value_part = kv_cache[..., HEAD_DIM:].astype(jnp.float32)
    scores = jnp.einsum('skqd,skld->skql', grouped, key_part) * HEAD_DIM ** (-0.5)
    draft_index = jnp.arange(per_group * DRAFT, dtype=jnp.int32) % DRAFT
    visible = lengths[:, None, None, None] - DRAFT + 1 + draft_index[None, None, :, None]
    position = jnp.arange(LEN, dtype=jnp.int32)
    allowed = position[None, None, None, :] < visible
    scores = jnp.where(allowed, scores, -1e+30)
    peak = lax.optimization_barrier(jnp.max(scores, axis=-1, keepdims=True))
    raised = jnp.exp(scores - peak)
    totals = lax.optimization_barrier(jnp.sum(raised, axis=-1, keepdims=True))
    weights = (raised / totals).astype(jnp.bfloat16)
    attended = jnp.einsum('skql,skld->skqd', weights.astype(jnp.float32), value_part).astype(jnp.bfloat16)
    attended = attended.reshape(seq_count, KV_HEADS, per_group, DRAFT, HEAD_DIM).transpose(0, 3, 1, 2, 4)
    return attended.reshape(seq_count, DRAFT, HEADS * HEAD_DIM)

def reference(queries, kv_cache, lengths, residual, out_weight, norm_gain):
    attended = attend(queries, kv_cache, lengths)
    flat_rows = attended.reshape(SEQS * DRAFT, HEADS * HEAD_DIM)
    columns = HEADS * HEAD_DIM // N_TP
    projected = jnp.zeros((SEQS * DRAFT, D), jnp.float32)
    for shard in range(N_TP):
        partial_term = jnp.dot(flat_rows[:, shard * columns:(shard + 1) * columns], out_weight[shard * columns:(shard + 1) * columns], preferred_element_type=jnp.float32)
        projected = projected + lax.optimization_barrier(partial_term.astype(jnp.bfloat16)).astype(jnp.float32)
    summed = residual.astype(jnp.float32) + projected.reshape(SEQS, DRAFT, D)
    hidden = summed.astype(jnp.bfloat16)
    scales = lax.rsqrt(lax.optimization_barrier(jnp.mean(summed * summed, axis=-1, keepdims=True)) + 1e-05)
    normed = (summed * scales * norm_gain.astype(jnp.float32)).astype(jnp.bfloat16)
    return (hidden, normed)
```

```python
import functools

import jax
import jax.numpy as jnp
from jax import lax
from jax.experimental import pallas as pl
from jax.experimental.pallas import tpu as pltpu
from jax.sharding import PartitionSpec as P

HEAD_DIM = 128
CHUNKS = 4
BLOCK_COLUMNS = 512


def attend_kernel(me_ref, lengths_ref, q_ref, kv_ref, out_ref, *, per_group):
    seq_count, draft, _ = q_ref.shape
    kv_heads, slots = kv_ref.shape[1], kv_ref.shape[2]
    head_columns = out_ref.shape[2]
    rows = per_group * draft
    token = lax.broadcasted_iota(jnp.int32, (rows, slots), 0) % draft
    position = lax.broadcasted_iota(jnp.int32, (rows, slots), 1)
    offset = position - token
    for seq in range(seq_count):
        allowed = offset < lengths_ref[seq] - draft + 1
        for head in range(kv_heads):
            first = head * per_group
            grouped = jnp.concatenate(
                [
                    q_ref[seq, :, (first + i) * HEAD_DIM:(first + i + 1) * HEAD_DIM]
                    for i in range(per_group)
                ],
                axis=0,
            )
            key_part = kv_ref[seq, head, :, :HEAD_DIM]
            value_part = kv_ref[seq, head, :, HEAD_DIM:]
            scores = lax.dot_general(
                grouped, key_part, (((1,), (1,)), ((), ())),
                preferred_element_type=jnp.float32,
            ) * HEAD_DIM ** (-0.5)
            scores = jnp.where(allowed, scores, -1e30)
            peak = jnp.max(scores, axis=-1, keepdims=True)
            raised = jnp.exp(scores - peak)
            totals = jnp.sum(raised, axis=-1, keepdims=True)
            weights = (raised / totals).astype(jnp.bfloat16)
            attended = jnp.dot(
                weights, value_part, preferred_element_type=jnp.float32
            ).astype(jnp.bfloat16)
            for i in range(per_group):
                column = (first + i) * HEAD_DIM
                slot, column = column // head_columns, column % head_columns
                out_ref[slot, seq * draft:(seq + 1) * draft, column:column + HEAD_DIM] = (
                    attended[i * draft:(i + 1) * draft]
                )


def attend(queries, kv_cache, lengths, me, tp):
    seq_count, draft, width = queries.shape
    kv_heads = kv_cache.shape[1]
    per_group = width // HEAD_DIM // kv_heads
    slots_per_step = max(1, tp // kv_heads)
    steps = tp // slots_per_step
    step_columns = width // steps
    step_kv_heads = kv_heads // steps

    def place(step, me_ref, lengths_ref):
        return step ^ (me_ref[0] // slots_per_step)

    return pl.pallas_call(
        functools.partial(attend_kernel, per_group=per_group),
        grid_spec=pltpu.PrefetchScalarGridSpec(
            num_scalar_prefetch=2,
            grid=(steps,),
            in_specs=[
                pl.BlockSpec((seq_count, draft, step_columns), lambda s, m, l: (0, 0, place(s, m, l))),
                pl.BlockSpec(
                    (seq_count, step_kv_heads) + kv_cache.shape[2:],
                    lambda s, m, l: (0, place(s, m, l), 0, 0),
                ),
            ],
            out_specs=pl.BlockSpec(
                (slots_per_step, seq_count * draft, width // tp), lambda s, m, l: (s, 0, 0)
            ),
        ),
        out_shape=jax.ShapeDtypeStruct((tp, seq_count * draft, width // tp), jnp.bfloat16),
        name="attend",
    )(me[None], lengths, queries, kv_cache)


def project_kernel(*refs, chunk, tp):
    row_refs, (weight, even_ref, odd_ref, blocks, sems) = refs[:tp], refs[tp:]
    count, _, columns = blocks.shape
    start = chunk * count * columns

    def copy(i):
        return pltpu.make_async_copy(
            weight.at[:, pl.ds(start + i * columns, columns)], blocks.at[i], sems.at[i]
        )

    for i in range(count):
        copy(i).start()
    order = list(range(0, tp, 2)) + list(range(1, tp, 2))
    rows = jnp.concatenate([row_refs[k][...] for k in order], axis=0)
    half = rows.shape[0] // 2
    for i in range(count):
        copy(i).wait()
        product = jnp.dot(rows, blocks[i], preferred_element_type=jnp.float32)
        even_ref[:, i * columns:(i + 1) * columns] = product[:half]
        odd_ref[:, i * columns:(i + 1) * columns] = product[half:].astype(jnp.bfloat16)


def project(row_blocks, weight, chunk, chunks):
    tp = len(row_blocks)
    half = row_blocks[0].shape[0] * tp // 2
    width = weight.shape[1] // chunks
    columns = min(BLOCK_COLUMNS, width)
    whole = pl.BlockSpec(memory_space=pltpu.VMEM)
    return pl.pallas_call(
        functools.partial(project_kernel, chunk=chunk, tp=tp),
        in_specs=[whole] * tp + [pl.BlockSpec(memory_space=pl.ANY)],
        out_specs=[whole, whole],
        out_shape=[
            jax.ShapeDtypeStruct((half, width), jnp.float32),
            jax.ShapeDtypeStruct((half, width), jnp.bfloat16),
        ],
        scratch_shapes=[
            pltpu.VMEM((width // columns, weight.shape[0], columns), jnp.bfloat16),
            pltpu.SemaphoreType.DMA((width // columns,)),
        ],
        cost_estimate=pl.CostEstimate(
            flops=4 * half * width * weight.shape[0],
            bytes_accessed=2 * width * weight.shape[0],
            transcendentals=0,
        ),
        name=f"project_{chunk}",
    )(*row_blocks, weight)


def finish_kernel(*refs, chunks, terms):
    groups, (residual, gain, hidden, normed) = refs[:-4], refs[-4:]
    seq_count, draft, width = residual.shape
    step = width // chunks
    rows = seq_count * draft
    squares = jnp.zeros((rows, 1), jnp.float32)
    parts = []
    for chunk in range(chunks):
        own, *others = groups[chunk * terms:(chunk + 1) * terms]
        columns = slice(chunk * step, (chunk + 1) * step)
        summed = own[...]
        for other in others:
            summed = summed + other[...].astype(jnp.float32)
        summed = summed + residual[:, :, columns].astype(jnp.float32).reshape(rows, step)
        hidden[:, :, columns] = summed.astype(jnp.bfloat16).reshape(seq_count, draft, step)
        squares = squares + jnp.sum(summed * summed, axis=-1, keepdims=True)
        parts.append(summed)
    scales = lax.rsqrt(squares / width + 1e-05)
    for chunk in range(chunks):
        columns = slice(chunk * step, (chunk + 1) * step)
        result = parts[chunk] * scales * gain[:, columns].astype(jnp.float32)
        normed[:, :, columns] = result.astype(jnp.bfloat16).reshape(seq_count, draft, step)


def exchange(value, tp, distance):
    return lax.ppermute(value, "tp", [(i, i ^ distance) for i in range(tp)])


def on_device(tp, queries, kv_cache, lengths, residual, out_weight, norm_gain):
    me = lax.axis_index("tp").astype(jnp.int32)
    rows = queries.shape[0] * queries.shape[1]
    attended = attend(queries, kv_cache, lengths, me, tp)
    low = max(1, tp // kv_cache.shape[1])
    if low > 1:
        picks = jnp.arange(tp, dtype=jnp.int32) ^ (me % low)
        attended = attended[picks]
    row_blocks = [attended[0]] + [exchange(attended[k], tp, k) for k in range(1, tp)]
    groups = []
    for chunk in range(CHUNKS):
        even, odd = project(row_blocks, out_weight, chunk, CHUNKS)
        paired = exchange(odd, tp, 1)
        terms = [even[:rows], paired[:rows]]
        for k in range(1, tp // 2):
            span = slice(k * rows, (k + 1) * rows)
            both = (even[span] + paired[span].astype(jnp.float32)).astype(jnp.bfloat16)
            terms.append(exchange(both, tp, 2 * k))
        groups.extend(terms)
    terms = len(groups) // CHUNKS
    out = jax.ShapeDtypeStruct(residual.shape, jnp.bfloat16)
    return tuple(pl.pallas_call(
        functools.partial(finish_kernel, chunks=CHUNKS, terms=terms),
        out_shape=[out, out],
        name="finish",
    )(*groups, residual, norm_gain[None]))


def solution(mesh):
    return jax.shard_map(
        functools.partial(on_device, mesh.shape["tp"]),
        mesh=mesh,
        in_specs=(
            P(("dp", "tp"), None, None),
            P(("dp", "tp"), None, None, None),
            P(("dp", "tp")),
            P(("dp", "tp"), None, None),
            P("tp", None),
            P(),
        ),
        out_specs=(P(("dp", "tp"), None, None), P(("dp", "tp"), None, None)),
        check_vma=False,
    )
```

```python
import functools

import jax
import jax.numpy as jnp
from jax import lax
from jax.experimental import pallas as pl
from jax.experimental.pallas import tpu as pltpu
from jax.sharding import PartitionSpec as P

HEAD_DIM = 128
CHUNKS = 4
BLOCK_COLUMNS = 512
VMEM_LIMIT = 24 * 2**20


def attend_kernel(me_ref, lengths_ref, q_ref, kv_ref, weight, *refs, per_group, tp):
    slot_refs, (fast_weight, block, sem) = refs[:tp], refs[tp:]
    step = pl.program_id(0)
    fetch = pltpu.make_async_copy(weight, fast_weight, sem)

    @pl.when(step == 0)
    def _():
        fetch.start()

    seq_count, draft, _ = q_ref.shape
    kv_heads, slots = kv_ref.shape[1], kv_ref.shape[2]
    slots_per_step, _, head_columns = block.shape
    rows = per_group * draft
    token = lax.broadcasted_iota(jnp.int32, (rows, slots), 0) % draft
    offset = lax.broadcasted_iota(jnp.int32, (rows, slots), 1) - token
    pairs = [(seq, head) for seq in range(seq_count) for head in range(kv_heads)]
    log2e = 1.4426950408889634
    scores, raised, totals = {}, {}, {}
    for seq, head in pairs:
        first = head * per_group
        grouped = jnp.concatenate(
            [
                q_ref[seq, :, (first + i) * HEAD_DIM:(first + i + 1) * HEAD_DIM]
                for i in range(per_group)
            ],
            axis=0,
        )
        product = lax.dot_general(
            grouped, kv_ref[seq, head, :, :HEAD_DIM], (((1,), (1,)), ((), ())),
            preferred_element_type=jnp.float32,
        )
        allowed = offset < lengths_ref[seq] - draft + 1
        scores[seq, head] = jnp.where(allowed, product, -1e30)
    for pair in pairs:
        peak = jnp.max(scores[pair], axis=-1, keepdims=True)
        powers = jnp.exp2((scores[pair] - peak) * (HEAD_DIM ** (-0.5) * log2e))
        totals[pair] = jnp.sum(powers, axis=-1, keepdims=True)
        raised[pair] = powers.astype(jnp.bfloat16)
    for seq, head in pairs:
        attended = jnp.dot(
            raised[seq, head], kv_ref[seq, head, :, HEAD_DIM:],
            preferred_element_type=jnp.float32,
        )
        attended = (attended * (1.0 / totals[seq, head])).astype(jnp.bfloat16)
        for i in range(per_group):
            column = (head * per_group + i) * HEAD_DIM
            slot, column = column // head_columns, column % head_columns
            block[slot, seq * draft:(seq + 1) * draft, column:column + HEAD_DIM] = (
                attended[i * draft:(i + 1) * draft]
            )
    for k in range(tp):
        @pl.when(step == k // slots_per_step)
        def _():
            slot_refs[k][...] = block[k % slots_per_step]

    @pl.when(step == pl.num_programs(0) - 1)
    def _():
        fetch.wait()


def attend(queries, kv_cache, lengths, weight, me, tp):
    seq_count, draft, width = queries.shape
    kv_heads = kv_cache.shape[1]
    per_group = width // HEAD_DIM // kv_heads
    slots_per_step = max(1, tp // kv_heads)
    steps = tp // slots_per_step
    step_columns = width // steps
    step_kv_heads = kv_heads // steps
    rows = seq_count * draft

    def place(step, me_ref):
        return step ^ (me_ref[0] // slots_per_step)

    slot_shape = (rows, width // tp)
    *slots, fast_weight = pl.pallas_call(
        functools.partial(attend_kernel, per_group=per_group, tp=tp),
        grid_spec=pltpu.PrefetchScalarGridSpec(
            num_scalar_prefetch=2,
            grid=(steps,),
            in_specs=[
                pl.BlockSpec((seq_count, draft, step_columns), lambda s, m, l: (0, 0, place(s, m))),
                pl.BlockSpec(
                    (seq_count, step_kv_heads) + kv_cache.shape[2:],
                    lambda s, m, l: (0, place(s, m), 0, 0),
                ),
                pl.BlockSpec(memory_space=pl.ANY),
            ],
            out_specs=[pl.BlockSpec(slot_shape, lambda s, m, l: (0, 0))] * tp
            + [pl.BlockSpec(memory_space=pltpu.VMEM)],
            scratch_shapes=[
                pltpu.VMEM((slots_per_step,) + slot_shape, jnp.bfloat16),
                pltpu.SemaphoreType.DMA,
            ],
        ),
        out_shape=[jax.ShapeDtypeStruct(slot_shape, jnp.bfloat16)] * tp
        + [pltpu.VMEM(weight.shape, weight.dtype)],
        compiler_params=pltpu.CompilerParams(vmem_limit_bytes=VMEM_LIMIT),
        name="attend",
    )(me[None], lengths, queries, kv_cache, weight)
    if slots_per_step > 1:
        picks = jnp.arange(tp, dtype=jnp.int32) ^ (me % slots_per_step)
        stacked = jnp.stack(slots)
        slots = [stacked[picks[k]] for k in range(tp)]
    return slots, fast_weight


def project_kernel(*refs, chunk, tp):
    row_refs, weight, own_ref, far_ref, odd_ref = refs[:tp], refs[tp], *refs[-3:]
    order = list(range(0, tp, 2)) + list(range(1, tp, 2))
    rows = jnp.concatenate([row_refs[k][...] for k in order], axis=0)
    one, half, width = own_ref.shape[0], odd_ref.shape[0], odd_ref.shape[1]
    columns = min(BLOCK_COLUMNS, width)
    for i in range(width // columns):
        span = slice(i * columns, (i + 1) * columns)
        start = chunk * width + i * columns
        product = jnp.dot(
            rows, weight[:, start:start + columns], preferred_element_type=jnp.float32
        )
        own_ref[:, span] = product[:one]
        far_ref[:, span] = product[one:half]
        odd_ref[:, span] = product[half:].astype(jnp.bfloat16)


def project(row_blocks, weight, chunk, chunks, after):
    tp = len(row_blocks)
    one = row_blocks[0].shape[0]
    half = one * tp // 2
    width = weight.shape[1] // chunks
    whole = pl.BlockSpec(memory_space=pltpu.VMEM)
    hbm = pl.BlockSpec(memory_space=pl.ANY)
    return pl.pallas_call(
        functools.partial(project_kernel, chunk=chunk, tp=tp),
        in_specs=[whole] * (tp + 1) + [hbm] * len(after),
        out_specs=[whole] * 3,
        out_shape=[
            jax.ShapeDtypeStruct((one, width), jnp.float32),
            jax.ShapeDtypeStruct((half - one, width), jnp.float32),
            jax.ShapeDtypeStruct((half, width), jnp.bfloat16),
        ],
        compiler_params=pltpu.CompilerParams(vmem_limit_bytes=VMEM_LIMIT),
        cost_estimate=pl.CostEstimate(
            flops=4 * half * width * weight.shape[0],
            bytes_accessed=2 * width * weight.shape[0],
            transcendentals=0,
        ),
        name=f"project_{chunk}",
    )(*row_blocks, weight, *after)


def finish_kernel(*refs, chunks, terms):
    groups, (residual, gain, hidden, normed) = refs[:-4], refs[-4:]
    seq_count, draft, width = residual.shape
    step = width // chunks
    rows = seq_count * draft
    squares = jnp.zeros((rows, 1), jnp.float32)
    parts = []
    for chunk in range(chunks):
        own, *others = groups[chunk * terms:(chunk + 1) * terms]
        columns = slice(chunk * step, (chunk + 1) * step)
        summed = own[...]
        for other in others:
            summed = summed + other[:rows].astype(jnp.float32)
        summed = summed + residual[:, :, columns].astype(jnp.float32).reshape(rows, step)
        hidden[:, :, columns] = summed.astype(jnp.bfloat16).reshape(seq_count, draft, step)
        squares = squares + jnp.sum(summed * summed, axis=-1, keepdims=True)
        parts.append(summed)
    scales = lax.rsqrt(squares / width + 1e-05)
    for chunk in range(chunks):
        columns = slice(chunk * step, (chunk + 1) * step)
        result = parts[chunk] * scales * gain[:, columns].astype(jnp.float32)
        normed[:, :, columns] = result.astype(jnp.bfloat16).reshape(seq_count, draft, step)


def exchange(value, tp, distance):
    return lax.ppermute(value, "tp", [(i, i ^ distance) for i in range(tp)])


def on_device(tp, queries, kv_cache, lengths, residual, out_weight, norm_gain):
    me = lax.axis_index("tp").astype(jnp.int32)
    rows = queries.shape[0] * queries.shape[1]
    slots, weight = attend(queries, kv_cache, lengths, out_weight, me, tp)
    weight = pltpu.with_memory_space_constraint(weight, pltpu.VMEM)
    row_blocks = [slots[0]] + [exchange(slots[k], tp, k) for k in range(1, tp)]
    groups, sent = [], []
    for chunk in range(CHUNKS):
        own, far, odd = project(row_blocks, weight, chunk, CHUNKS, sent[-2] if len(sent) > 1 else [])
        paired = exchange(odd, tp, 1)
        sums = [
            (far[(k - 1) * rows:k * rows] + paired[k * rows:(k + 1) * rows].astype(jnp.float32))
            .astype(jnp.bfloat16)
            for k in range(1, tp // 2)
        ]
        sent.append(sums)
        groups.extend([own, paired] + [exchange(both, tp, 2 * k + 2) for k, both in enumerate(sums)])
    terms = len(groups) // CHUNKS
    out = jax.ShapeDtypeStruct(residual.shape, jnp.bfloat16)
    return tuple(pl.pallas_call(
        functools.partial(finish_kernel, chunks=CHUNKS, terms=terms),
        out_shape=[out, out],
        name="finish",
    )(*groups, residual, norm_gain[None]))


def solution(mesh):
    return jax.shard_map(
        functools.partial(on_device, mesh.shape["tp"]),
        mesh=mesh,
        in_specs=(
            P(("dp", "tp"), None, None),
            P(("dp", "tp"), None, None, None),
            P(("dp", "tp")),
            P(("dp", "tp"), None, None),
            P("tp", None),
            P(),
        ),
        out_specs=(P(("dp", "tp"), None, None), P(("dp", "tp"), None, None)),
        check_vma=False,
    )
```
